512 devices in a mesh: bx: 32 (over z_hi, y, x), by: 16 (over z_lo, core).
Axes of the slice: x: 4, y: 4, z: 16 (z_hi: 2, z_lo: 8; z = z_hi * 8 + z_lo), core: 2. Of those that a mesh axis runs over, the one named last changes fastest.
Arguments:
- occ_factor: bfloat16 [32, 16, 20, 256], P('bx', 'by'), may hold values from -6 to 6
- coefficients: bfloat16 [32, 16, 9, 20, 1600], P('bx', 'by'), may hold values from -0.4375 to 0.4375
- coulomb: bfloat16 [32, 16, 9, 80, 80], P('bx', 'by'), may hold values from -0.0390625 to 0.0390625
- box_pair_mask: int32 [32, 16, 9], P('bx', 'by'), may hold values 0 or 1
- live_count: int32 [32, 16], P('bx', 'by'), may hold values from 5 to 20
Outputs:
- exchange: float32 [32, 16, 9, 20, 20], P('bx', 'by')
The draws below stay inside these ranges and needn't reach their ends.
All inputs are finite; a program needn't handle non-finite values. No bound on the sum of `box_pair_mask` on one device may be relied on, other than what follows from the above.
Results may differ from the reference program's by a relative error of at most 0.003.
Values may be sent and summed in bfloat16 or wider, within the bound.
No kernel may reach another device: no remote copies, remote signals or barrier semaphores. Data moves between devices by JAX's collectives and lax.ppermute only.
A program may use at most 64 MiB of HBM per device.

```python
import jax
import jax.numpy as jnp
from jax import lax

OCCUPIED_COUNT = 256
PAIR_SLOTS = 9
PADDED_BASIS = 20
AUX_FUNCTIONS = 80
BOXES_FIRST_DIM = 32
BOXES_SECOND_DIM = 16


def plant(entries, rng, least, largest):
    index_at = [jax.random.randint(jax.random.fold_in(rng, axis), (), 0, length) for axis, length in enumerate(entries.shape)]
    main_axis = entries.shape.index(max(entries.shape))
    next_to = index_at[:main_axis] + [(index_at[main_axis] + 1) % entries.shape[main_axis]] + index_at[main_axis + 1:]
    return entries.at[tuple(index_at)].set(least).at[tuple(next_to)].set(largest)


def levels(stream_key, extent, shards, smallest, largest):
    def one(axis_at, parts):
        draws = jax.random.uniform(jax.random.fold_in(jax.random.fold_in(stream_key, 6), axis_at), (parts,), jnp.float32, smallest / len(shards), largest / len(shards))
        return jnp.repeat(jnp.exp(draws), extent[axis_at] // parts).reshape((-1,) + (1,) * (len(extent) - axis_at - 1))

    factor_of = one(*shards[0])
    for cut in shards[1:]:
        factor_of = factor_of * one(*cut)
    return factor_of


def noise(key, extent, spread, reach, cuts=(), held_as=jnp.bfloat16):
    loudness = levels(key, extent, cuts, -0.22, 0.18) if cuts else 1.0
    entries = jax.random.normal(key, extent, jnp.float32) * spread * loudness
    return jnp.minimum(jnp.maximum(entries, -reach), reach).astype(held_as)


def setup_inputs(seed: int = 0) -> dict:
    key_of = jax.random.split(jax.random.key(seed), 6)
    occ_factor = noise(key_of[0], (BOXES_FIRST_DIM, BOXES_SECOND_DIM, PADDED_BASIS, OCCUPIED_COUNT), 1.0, 6.0, ((0, 32), (1, 16)))
    coefficients = noise(key_of[1], (BOXES_FIRST_DIM, BOXES_SECOND_DIM, PAIR_SLOTS, PADDED_BASIS, AUX_FUNCTIONS * PADDED_BASIS), (PAIR_SLOTS * PADDED_BASIS) ** -0.5, 0.4375, ((0, 32), (1, 16)))
    coulomb = noise(key_of[2], (BOXES_FIRST_DIM, BOXES_SECOND_DIM, PAIR_SLOTS, AUX_FUNCTIONS, AUX_FUNCTIONS), (AUX_FUNCTIONS * OCCUPIED_COUNT) ** -0.5, 0.0390625, ((0, 32), (1, 16)))
    box_pair_mask = plant((jax.random.randint(key_of[3], (BOXES_FIRST_DIM, BOXES_SECOND_DIM, PAIR_SLOTS), 0, 4) < 3).astype(jnp.int32), jax.random.fold_in(key_of[3], 1), 0, 1)
    live_count = plant(jax.random.randint(key_of[4], (BOXES_FIRST_DIM, BOXES_SECOND_DIM), PADDED_BASIS // 4, PADDED_BASIS + 1), jax.random.fold_in(key_of[4], 1), PADDED_BASIS // 4, PADDED_BASIS).astype(jnp.int32)
    return {"occ_factor": occ_factor, "coefficients": coefficients, "coulomb": coulomb, "box_pair_mask": box_pair_mask, "live_count": live_count}


def reference(occ_factor, coefficients, coulomb, box_pair_mask, live_count):
    basis_rows = jnp.arange(PADDED_BASIS, dtype=jnp.int32)
    row_live = (basis_rows[None, None, :, None] < live_count[:, :, None, None]).astype(jnp.float32)
    masked = (occ_factor.astype(jnp.float32) * row_live).astype(jnp.bfloat16)
    own_box_slot = (jnp.arange(PAIR_SLOTS, dtype=jnp.int32) == PAIR_SLOTS // 2).astype(jnp.int32)
    pair_on = jnp.maximum(box_pair_mask, own_box_slot[None, None, :])
    column_basis = jnp.arange(AUX_FUNCTIONS * PADDED_BASIS, dtype=jnp.int32) % PADDED_BASIS
    column_live = (column_basis[None, None, None, None, :] < live_count[:, :, None, None, None]).astype(jnp.float32)
    keep_factor = pair_on[:, :, :, None, None].astype(jnp.float32) * column_live
    coef_kept = (coefficients.astype(jnp.float32) * keep_factor).astype(jnp.bfloat16)
    padded = jnp.pad(masked, ((1, 1), (1, 1), (0, 0), (0, 0)))

    def fit_row(inputs):
        coef_row, row_index = inputs
        window = lax.dynamic_slice_in_dim(padded, row_index, 3, 0)
        nearby = jnp.stack([window[row_off, col_off:col_off + BOXES_SECOND_DIM] for row_off in range(3) for col_off in range(3)], axis=1)
        fitted_row = jnp.einsum("ysna,ysnj->yaj", coef_row.astype(jnp.float32), nearby.astype(jnp.float32))
        return fitted_row.astype(jnp.bfloat16)

    fitted = lax.map(fit_row, (coef_kept, jnp.arange(BOXES_FIRST_DIM, dtype=jnp.int32)))
    fitted_pad = jnp.pad(fitted, ((1, 1), (1, 1), (0, 0), (0, 0)))

    def exchange_row(inputs):
        coul_row, own_row, pair_row, row_index = inputs
        window = lax.dynamic_slice_in_dim(fitted_pad, row_index, 3, 0)
        own_split = own_row.reshape(BOXES_SECOND_DIM, AUX_FUNCTIONS, PADDED_BASIS * OCCUPIED_COUNT).astype(jnp.float32)
        blocks = []
        for neighbour_index in range(PAIR_SLOTS):
            row_off, col_off = divmod(neighbour_index, 3)
            nearby = window[row_off, col_off:col_off + BOXES_SECOND_DIM].reshape(BOXES_SECOND_DIM, AUX_FUNCTIONS, PADDED_BASIS, OCCUPIED_COUNT)
            applied = jnp.einsum("yqp,ypk->yqk", coul_row[:, neighbour_index].astype(jnp.float32), own_split).astype(jnp.bfloat16)
            blocks.append(jnp.einsum("yqmi,yqni->ymn", applied.reshape(BOXES_SECOND_DIM, AUX_FUNCTIONS, PADDED_BASIS, OCCUPIED_COUNT).astype(jnp.float32), nearby.astype(jnp.float32)))
        stacked = jnp.stack(blocks, axis=1)
        return -0.25 * pair_row[:, :, None, None].astype(jnp.float32) * stacked

    return lax.map(exchange_row, (coulomb, fitted, pair_on, jnp.arange(BOXES_FIRST_DIM, dtype=jnp.int32)))
```

```python
import functools

import jax
import jax.numpy as jnp
from jax import lax
from jax.experimental import pallas as pl
from jax.experimental.pallas import tpu as pltpu
from jax.sharding import PartitionSpec as P

BF = jnp.bfloat16
F32 = jnp.float32
OWN_SLOTS = (1, 3, 4, 5, 7)
GROUP = 8
VMEM = pl.BlockSpec(memory_space=pltpu.VMEM)
SMEM = pl.BlockSpec(memory_space=pltpu.SMEM)


def call(body, outs, n_smem, n_vmem, scratch, flops):
    return pl.pallas_call(
        body,
        out_shape=outs,
        in_specs=[SMEM] * n_smem + [VMEM] * n_vmem,
        out_specs=jax.tree.map(lambda _: VMEM, outs),
        scratch_shapes=scratch,
        cost_estimate=pl.CostEstimate(flops=flops, bytes_accessed=1000000, transcendentals=0),
    )


def prep_kernel(live_ref, pair_ref, coef_ref, k_ref, *rest):
    *piece_refs, kf = rest
    slots, basis, cols = coef_ref.shape
    col = lax.broadcasted_iota(jnp.int32, (1, cols), 1) % basis
    keep = (col < live_ref[0]).astype(F32)
    for s in range(slots):
        on = 1.0 if s == slots // 2 else pair_ref[s].astype(F32)
        kf[s * basis : (s + 1) * basis, :] = coef_ref[s].astype(F32) * (keep * on)
    used = slots * basis
    kf[used:, :] = jnp.zeros((kf.shape[0] - used, cols), F32)
    k_ref[...] = kf[...].astype(BF)
    at = 0
    for piece in piece_refs:
        piece[...] = kf[at : at + piece.shape[0], :].astype(BF)
        at += piece.shape[0]


def load_window(cols_refs, rows, wf, outer=None, far=None):
    basis = cols_refs[0].shape[1]
    for s in range(9):
        dr, dc = divmod(s, 3)
        if rows[dr] is None:
            block = outer[dc].astype(F32)
            block = jnp.where(far, cols_refs[dc][3].astype(F32), block)
        else:
            block = cols_refs[dc][rows[dr]].astype(F32)
        wf[s * basis : (s + 1) * basis, :] = block
    wf[9 * basis :, :] = jnp.zeros((wf.shape[0] - 9 * basis, wf.shape[1]), F32)
    return wf[...].astype(BF)


def fit_into(k_ref, window, out_ref):
    total = k_ref.shape[1]
    for at in range(0, total, 256):
        width = min(256, total - at)
        out_ref[at : at + width, :] = lax.dot_general(
            k_ref[:, at : at + width], window, (((0,), (0,)), ((), ())), preferred_element_type=F32
        ).astype(out_ref.dtype)


def own_fit_kernel(k_ref, ml_ref, mc_ref, mr_ref, c_ref, out_ref, wf):
    window = load_window((ml_ref, mc_ref, mr_ref), (0, 1, 2), wf)
    fit_into(k_ref, window, out_ref)
    total = k_ref.shape[1]
    aux = c_ref.shape[1]
    for at, (one, two) in ((total, (0, 6)), (total + aux, (2, 8))):
        out_ref[at : at + aux, :] = jnp.zeros((aux, out_ref.shape[1]), BF)
        out_ref[at : at + aux, 0:aux] = c_ref[one]
        out_ref[at : at + aux, 128 : 128 + aux] = c_ref[two]


def side_fit_kernel(rows, flag_ref, k_ref, b1_ref, b2_ref, b3_ref, ml_ref, mc_ref, mr_ref, o_ref, out_ref, wf, kk):
    far = flag_ref[0] > 0
    window = load_window((ml_ref, mc_ref, mr_ref), rows, wf, o_ref, far)

    @pl.when(far)
    def _():
        at = 0
        for piece in (b1_ref, b2_ref, b3_ref):
            kk[at : at + piece.shape[0], :] = piece[...]
            at += piece.shape[0]

    @pl.when(jnp.logical_not(far))
    def _():
        kk[...] = k_ref[...]

    fit_into(kk, window, out_ref)


def apply_into(blocks, f_ref, fs, xs):
    aux = blocks[0].shape[0]
    halves, total, lanes = fs.shape
    basis = total // aux
    for h in range(halves):
        fs[h] = f_ref[0:total, h * lanes : (h + 1) * lanes].astype(F32)
    stack = jnp.concatenate(blocks, axis=0) if len(blocks) > 1 else blocks[0]
    for m in range(basis):
        rows = pl.ds(m, aux, stride=basis)
        part = jnp.concatenate([fs.at[h][rows, :] for h in range(halves)], axis=1).astype(BF)
        res = jnp.dot(stack, part, preferred_element_type=F32)
        for t in range(len(blocks)):
            for h in range(halves):
                xs.at[t, h][rows, :] = res[t * aux : (t + 1) * aux, h * lanes : (h + 1) * lanes]


def contract(lefts, right, basis):
    step = GROUP * basis
    acc = [jnp.zeros((step, step), F32) for _ in lefts]
    for at in range(0, 1600, step):
        rhs = right(at, step)
        for i, left in enumerate(lefts):
            acc[i] = acc[i] + lax.dot_general(
                left(at, step), rhs, (((1,), (1,)), ((), ())), preferred_element_type=F32
            )
    row = lax.broadcasted_iota(jnp.int32, (step, step), 0) // basis
    col = lax.broadcasted_iota(jnp.int32, (step, step), 1) // basis
    fold = (
        lax.broadcasted_iota(jnp.int32, (step, basis), 0) % basis
        == lax.broadcasted_iota(jnp.int32, (step, basis), 1)
    ).astype(F32)
    outs = []
    for a in acc:
        a = jnp.where(row == col, a, 0.0)
        flat = a[0:basis]
        for j in range(1, GROUP):
            flat = flat + a[j * basis : (j + 1) * basis]
        outs.append(jnp.dot(flat, fold, preferred_element_type=F32, precision=lax.Precision.HIGHEST))
    return outs


def own_apply_kernel(f_ref, c_ref, x_ref, e_ref, fs, xs):
    apply_into([c_ref[s] for s in OWN_SLOTS], f_ref, fs, xs)
    for t in range(len(OWN_SLOTS)):
        for h in range(2):
            x_ref[t, :, h * 128 : (h + 1) * 128] = xs[t, h].astype(BF)
    basis = e_ref.shape[0]
    (e_ref[...],) = contract(
        [lambda at, n: x_ref[2, at : at + n, :]], lambda at, n: f_ref[at : at + n, :], basis
    )


def rows_of(ref, *lead):
    return lambda at, n: ref[(*lead, slice(at, at + n), slice(None))]


def near_apply_kernel(fl_ref, fr_ref, x_ref, xl_ref, xr_ref, el_ref, er_ref, fs, xs):
    basis = el_ref.shape[0]
    total = xl_ref.shape[1]
    aux = total // basis
    for ref, start, out in ((fl_ref, total + aux, xl_ref), (fr_ref, total, xr_ref)):
        apply_into([ref[start : start + aux, at : at + aux] for at in (0, 128)], ref, fs, xs)
        for t in range(2):
            for h in range(2):
                out[t, :, h * 128 : (h + 1) * 128] = xs[t, h].astype(BF)
    (el_ref[...],) = contract([rows_of(x_ref, 1)], rows_of(fl_ref), basis)
    (er_ref[...],) = contract([rows_of(x_ref, 3)], rows_of(fr_ref), basis)


def pairs_kernel(x_ref, xl_ref, xr_ref, up_ref, dn_ref, own_ref, lo_ref, hi_ref):
    basis = own_ref.shape[1]
    for i, (t, ref) in enumerate(((0, up_ref), (4, dn_ref))):
        own_ref[i], lo_ref[i], hi_ref[i] = contract(
            [rows_of(x_ref, t), rows_of(xl_ref, i), rows_of(xr_ref, i)], rows_of(ref), basis
        )


def join_kernel(pair_ref, left_ref, right_ref, own_ref, ec_ref, el_ref, er_ref, out_ref):
    parts = [
        left_ref[0], own_ref[0], right_ref[0], el_ref[...], ec_ref[...], er_ref[...],
        left_ref[1], own_ref[1], right_ref[1],
    ]
    for s, part in enumerate(parts):
        on = 1.0 if s == 4 else pair_ref[s].astype(F32)
        out_ref[s] = part * (-0.25 * on)


def steps(n, by, skip=None):
    return [(i, i + by) for i in range(n) if 0 <= i + by < n and {i, i + by} != skip]


def move(x, axis, pairs):
    return lax.ppermute(x, axis, pairs)


def m_kernel(live_ref, occ_ref, m_ref):
    rows = lax.broadcasted_iota(jnp.int32, occ_ref.shape, 0)
    m_ref[...] = jnp.where(rows < live_ref[0], occ_ref[...].astype(F32), 0.0).astype(BF)


def column_kernel(where_ref, up_ref, m_ref, dn_ref, edge_ref, out_ref):
    seam = edge_ref[0].astype(F32)
    out_ref[0] = jnp.where(where_ref[0] > 0, seam, up_ref[...].astype(F32)).astype(BF)
    out_ref[1] = m_ref[...]
    out_ref[2] = jnp.where(where_ref[1] > 0, seam, dn_ref[...].astype(F32)).astype(BF)
    out_ref[3] = edge_ref[1]


def body(occ_factor, coefficients, coulomb, box_pair_mask, live_count):
    basis, orbitals = occ_factor.shape[2:]
    aux = coulomb.shape[3]
    total = aux * basis
    depth = 192
    c = coulomb[0, 0]
    nx, ny = lax.axis_size("bx"), lax.axis_size("by")
    low, high = nx // 2 - 1, nx // 2
    seam = {low, high}
    sds = jax.ShapeDtypeStruct
    live, pair = live_count.reshape(1), box_pair_mask[0, 0]
    m = call(m_kernel, sds((basis, orbitals), BF), 1, 1, [], 10**5)(live, occ_factor[0, 0])
    row = lax.axis_index("bx")
    m_up = move(m, "bx", steps(nx, 1, seam))
    m_dn = move(m, "bx", steps(nx, -1, seam))
    (one, two), *relays = [(12, 19), (3, 28), (14, 17), (11, 20)]
    edge = jnp.stack([m, jnp.where(row == low, m_up, m_dn)])
    edge = move(edge, "bx", [(low, one), (high, two)])
    edge = move(edge, "bx", [(one, high), (two, low)])
    k, *kb = call(
        prep_kernel,
        (sds((depth, total), BF), *[sds((64, total), BF)] * 3),
        2, 1, [pltpu.VMEM((depth, total), F32)], 10**7,
    )(live, pair, coefficients[0, 0])
    hops = [move(kb[j], "bx", [(low, one), (high, two)]) for j, (one, two) in enumerate(relays)]
    k_up = move(k, "bx", steps(nx, 1, seam))
    k_dn = move(k, "bx", steps(nx, -1, seam))
    far = [move(hops[j], "bx", [(one, high), (two, low)]) for j, (one, two) in enumerate(relays)]
    where = jnp.stack([row == high, row == low]).astype(jnp.int32)
    column = call(column_kernel, sds((4, basis, orbitals), BF), 1, 4, [], 10**5)(where, m_up, m, m_dn, edge)
    ml = move(column, "by", steps(ny, 1))
    mr = move(column, "by", steps(ny, -1))
    windows = (ml, column, mr)
    wf = pltpu.VMEM((depth, orbitals), F32)
    fit_flops = 2 * depth * total * orbitals
    f = call(own_fit_kernel, sds((total + 2 * aux, orbitals), BF), 0, 5, [wf], fit_flops)(k, *windows, c)
    fl = move(f, "by", steps(ny, 1))
    fr = move(f, "by", steps(ny, -1))
    big = pltpu.VMEM((2, total, 128), F32)
    x, e_c = call(
        own_apply_kernel,
        (sds((5, total, orbitals), BF), sds((basis, basis), F32)),
        0, 2, [big, pltpu.VMEM((5, 2, total, 128), F32)], 10 * aux * total * orbitals,
    )(f, c)
    row = lax.axis_index("bx")
    upper = move(jnp.stack([ml[0], column[0], mr[0]]), "bx", steps(nx, 1, seam))
    lower = move(jnp.stack([ml[2], column[2], mr[2]]), "bx", steps(nx, -1, seam))
    side = []
    for rows, mine, outer, at in (((None, 0, 1), k_up, upper, high), ((1, 2, None), k_dn, lower, low)):
        flag = (row == at).astype(jnp.int32).reshape(1)
        side.append(call(
            functools.partial(side_fit_kernel, rows), sds((total, orbitals), BF), 1, 8,
            [wf, pltpu.VMEM((depth, total), BF)], fit_flops,
        )(flag, mine, *far, *windows, outer))
    xl, xr, e_l, e_r = call(
        near_apply_kernel,
        (sds((2, total, orbitals), BF),) * 2 + (sds((basis, basis), F32),) * 2,
        0, 3, [big, pltpu.VMEM((2, 2, total, 128), F32)], 10 * aux * total * orbitals,
    )(fl, fr, x)
    own, lo, hi = call(
        pairs_kernel, (sds((2, basis, basis), F32),) * 3, 0, 5, [], 10 * aux * total * orbitals,
    )(x, xl, xr, *side)
    from_right = move(lo, "by", steps(ny, -1))
    from_left = move(hi, "by", steps(ny, 1))
    out = call(
        join_kernel, sds((9, basis, basis), F32), 1, 6, [], 10**5,
    )(pair, from_left, from_right, own, e_c, e_l, e_r)
    return out[None, None]


def solution(mesh):
    in_specs = (
        P("bx", "by", None, None),
        P("bx", "by", None, None, None),
        P("bx", "by", None, None, None),
        P("bx", "by", None),
        P("bx", "by"),
    )
    out_specs = P("bx", "by", None, None, None)
    return jax.shard_map(body, mesh=mesh, in_specs=in_specs, out_specs=out_specs, check_vma=False)
```
